32 devices in a mesh: dp: 16 (over z, y, x), head: 2 (over core).
Axes of the slice: x: 2, y: 2, z: 4, core: 2. Of those that a mesh axis runs over, the one named last changes fastest.
Arguments:
- tokens: bfloat16 [16384, 768], P(('dp', 'head')), may hold values from -6 to 6
- mixer_gain: float32 [768], replicated, may hold values from 0.1 to 1.9
- joined_weight: bfloat16 [768, 2304], replicated, may hold values from -0.21875 to 0.21875
- merge_weight: bfloat16 [768, 768], replicated, may hold values from -0.875 to 0.875
- feeder_gain: float32 [768], replicated, may hold values from 0.1 to 1.9
- expand_weight: bfloat16 [768, 2304], replicated, may hold values from -0.21875 to 0.21875
- shrink_weight: bfloat16 [1152, 768], replicated, may hold values from -0.1875 to 0.1875
- doc_lengths: int32 [16, 4], P('dp'), may hold values from 1 to 512, 1024 in all within a row
- padding: int32 [16], P('dp'), may hold values from 0 to 255
- cotangent: bfloat16 [16384, 768], P(('dp', 'head')), may hold values from -6 to 6
Outputs:
- block_output: bfloat16 [16384, 768], P(('dp', 'head'))
- tokens_gradient: bfloat16 [16384, 768], P(('dp', 'head'))
- mixer_gradient: float32 [768], P('head')
- joined_gradient: float32 [768, 2304], P('head')
- merge_gradient: float32 [768, 768], P('head')
- feeder_gradient: float32 [768], P('head')
- expand_gradient: float32 [768, 2304], P('head')
- shrink_gradient: float32 [1152, 768], P('head')
The draws below stay inside these ranges and needn't reach their ends.
Inputs may be any that keep to these rules, and one draw needn't show every extreme that they name: `doc_lengths`: each slot's 4 lengths are positive, sum to 1024, and the longest is exactly 512.
All inputs are finite; a program needn't handle non-finite values.
Results may differ from the reference program's by a relative error of at most 0.013.
Values may be sent and summed in bfloat16 or wider, within the bound.
A program may use at most 192 MiB of HBM per device.

```python
import math
import jax
import jax.numpy as jnp
import numpy as np
from jax import lax

D = 768
HEADS = 12
HD = 64
FF = 1152
SLOT = 1024
DOCS = 4
TOKENS = 16384
SLOTS = 16


def plant(values, own_key, smallest, top_value):
    longest = values.shape.index(max(values.shape))
    spots = []
    for shift in (0, 1):
        where = [jax.random.randint(jax.random.fold_in(own_key, axis), (), 0, length) for axis, length in enumerate(values.shape)]
        where[longest] = (where[longest] + shift) % values.shape[longest]
        spots.append(tuple(where))
    return values.at[spots[0]].set(smallest).at[spots[1]].set(top_value)


def block_scale(stream_key, extent, split, low, high):
    def one(dim, shards_of):
        heights = jax.random.uniform(jax.random.fold_in(jax.random.fold_in(stream_key, 6), dim), (shards_of,), jnp.float32, low / len(split), high / len(split))
        return jnp.repeat(jnp.exp(heights), extent[dim] // shards_of).reshape((-1,) + (1,) * (len(extent) - dim - 1))

    level = one(*split[0])
    for cut in split[1:]:
        level = level * one(*cut)
    return level


def length_profile(amount, total, bound, slope):
    loads = [(1 << 20) // math.isqrt(grade ** slope) + 1 for grade in range(2, amount + 1)]
    rest, given = total - bound - (amount - 1), [1] * (amount - 1)
    while rest > 0:
        movable = [i for i in range(amount - 1) if given[i] < bound]
        whole, remaining = sum([loads[i] for i in movable]), rest
        for i in movable:
            more = min(bound - given[i], max(1, remaining * loads[i] // whole), rest)
            given[i] = given[i] + more
            rest = rest - more
    return np.array([bound] + given)


def uneven(rng, amount, total, bound, lean):
    if amount == 2:
        one = jax.random.randint(rng, (), max(1, total - bound), min(bound, total - 1) + 1)
        return jnp.stack([one, total - one])
    lengths = jnp.asarray(length_profile(amount, total, bound, lean), jnp.int32)
    twos = (amount - 1) // 2
    source_of, taker = lengths[1:1 + 2 * twos:2], lengths[2:2 + 2 * twos:2]
    room = jnp.minimum(source_of - 1, bound - taker)
    moved = jax.random.randint(jax.random.fold_in(rng, 1), (twos,), 0, 1 << 20) % (room + 1)
    lengths = lengths.at[1:1 + 2 * twos:2].set(source_of - moved).at[2:2 + 2 * twos:2].set(taker + moved)
    return lengths[jax.random.permutation(jax.random.fold_in(rng, 2), amount)]


def bell_draw(key, shape, width, limit, cuts=(), held_as=jnp.bfloat16):
    entries = width * jax.random.normal(key, shape, jnp.float32)
    if cuts:
        entries = entries * block_scale(key, shape, cuts, -0.22, 0.18)
    return jnp.clip(entries, -limit, limit).astype(held_as)


def setup_inputs(seed: int = 0) -> dict:
    splits = jax.random.split(jax.random.key(seed), 11)
    return {
        "tokens": bell_draw(splits[0], (TOKENS, D), 1.0, 6.0, ((0, 32),)),
        "mixer_gain": jnp.clip(1.0 + 0.18 * jax.random.normal(splits[1], (D,), jnp.float32), 0.1, 1.9),
        "joined_weight": bell_draw(splits[2], (D, 3 * D), D ** -0.5, 0.21875),
        "merge_weight": bell_draw(splits[3], (D, D), (D // 16) ** -0.5, 0.875),
        "feeder_gain": jnp.clip(1.0 + 0.18 * jax.random.normal(splits[4], (D,), jnp.float32), 0.1, 1.9),
        "expand_weight": bell_draw(splits[5], (D, 2 * FF), D ** -0.5, 0.21875),
        "shrink_weight": bell_draw(splits[6], (FF, D), FF ** -0.5, 0.1875),
        "doc_lengths": jax.vmap(lambda own: uneven(own, DOCS, SLOT, SLOT // 2, 2))(jax.random.split(splits[7], SLOTS)).reshape((SLOTS, DOCS)).astype(jnp.int32),
        "padding": plant(jax.random.randint(splits[8], (SLOTS,), 0, SLOT // 4), jax.random.fold_in(splits[8], 1), 0, (SLOT // 4) - 1).astype(jnp.int32),
        "cotangent": bell_draw(splits[9], (TOKENS, D), 1.0, 6.0, ((0, 32),)),
    }


@jax.custom_vjp
def low(v):
    return lax.optimization_barrier(v.astype(jnp.bfloat16)).astype(jnp.float32)

@jax.custom_vjp
def low_back(v):
    return v

def low_keep(v):
    return (low(v), None)

def low_pass(kept, grad):
    return (grad,)

def back_keep(v):
    return (v, None)

def back_low(kept, grad):
    return (low(grad),)
low.defvjp(low_keep, low_pass)
low_back.defvjp(back_keep, back_low)
epsilon = 1e-05
rotary_base = 160000.0
masked_score = -1e+30

def highest(left, right):
    return jnp.dot(left, right, precision=lax.Precision.HIGHEST)

def normalize(values, gain):
    centred = values - lax.optimization_barrier(jnp.mean(values, axis=-1, keepdims=True))
    factor = lax.rsqrt(lax.optimization_barrier(jnp.mean(centred * centred, axis=-1, keepdims=True)) + epsilon)
    return centred * factor * gain

def slot_layout(lengths_row, padding_row):
    places = jnp.arange(SLOT, dtype=jnp.int32)
    bounds = jnp.cumsum(lengths_row).astype(jnp.int32)
    passed = (places[:, None] >= bounds[None, :]).astype(jnp.int32)
    segment = lax.optimization_barrier(jnp.sum(passed, axis=1)).astype(jnp.int32)
    start = lax.optimization_barrier(jnp.sum(passed * lengths_row[None, :], axis=1)).astype(jnp.int32)
    position = (places - start).astype(jnp.float32)
    kept = jnp.logical_not(places >= SLOT - padding_row)
    allowed = (segment[:, None] == segment[None, :]) & kept[:, None] & kept[None, :]
    allowed = allowed | (places[:, None] == places[None, :])
    return (position, allowed)

def turning(position):
    halfway = HD // 2
    rates = jnp.exp(jnp.arange(halfway, dtype=jnp.float32) * (-2.0 * math.log(rotary_base) / HD))
    angles = position[:, None] * rates[None, :]
    doubled = jnp.concatenate([angles, angles], axis=1)
    return (jnp.cos(doubled), jnp.sin(doubled))

def rotate(values, cosine, sine):
    halfway = values.shape[-1] // 2
    turned = jnp.concatenate([-values[..., halfway:], values[..., :halfway]], axis=-1)
    return values * cosine[:, None, :] + turned * sine[:, None, :]

def attend_slot(item):
    packed, lengths_row, padding_row = item
    position, allowed = slot_layout(lengths_row, padding_row)
    cosine, sine = turning(position)
    queries = low(rotate(packed[:, 0], cosine, sine))
    keys = low(rotate(packed[:, 1], cosine, sine))
    values = packed[:, 2]
    scores = jnp.einsum('qhd,khd->hqk', queries, keys, precision=lax.Precision.HIGHEST) * HD ** (-0.5)
    scores = low_back(scores)
    scores = jnp.where(allowed[None], scores, masked_score)
    top = lax.optimization_barrier(jnp.max(scores, axis=-1, keepdims=True))
    weights = jnp.exp(scores - top)
    probs = weights / lax.optimization_barrier(jnp.sum(weights, axis=-1, keepdims=True))
    mixed = jnp.einsum('hqk,khd->qhd', low(probs), values, precision=lax.Precision.HIGHEST)
    return low_back(low(mixed))

def forward(inputs, mixer_gain, joined_weight, merge_weight, feeder_gain, expand_weight, shrink_weight, doc_lengths, padding):
    first_in = low(normalize(inputs, mixer_gain))
    joined = low_back(low(highest(first_in, joined_weight)))
    packed = joined.reshape(SLOTS, SLOT, 3, HEADS, HD)
    mixed = lax.map(jax.checkpoint(attend_slot), (packed, doc_lengths, padding))
    mixed = mixed.reshape(TOKENS, D)
    residual = inputs + low_back(highest(mixed, merge_weight))
    second_in = low(normalize(residual, feeder_gain))
    expanded = low_back(highest(second_in, expand_weight))
    hidden = low(jax.nn.gelu(expanded[:, :FF], approximate=False) * expanded[:, FF:])
    return residual + highest(hidden, shrink_weight)

def reference(tokens, mixer_gain, joined_weight, merge_weight, feeder_gain, expand_weight, shrink_weight, doc_lengths, padding, cotangent):
    floats = tuple((value.astype(jnp.float32) for value in (tokens, mixer_gain, joined_weight, merge_weight, feeder_gain, expand_weight, shrink_weight)))

    def closed(*values):
        return forward(*values, doc_lengths, padding)
    result, pull = jax.vjp(closed, *floats)
    changes = pull(cotangent.astype(jnp.float32))
    return (result.astype(jnp.bfloat16), changes[0].astype(jnp.bfloat16), changes[1], changes[2], changes[3], changes[4], changes[5], changes[6])
```

```python
import functools
import math

import jax
import jax.numpy as jnp
from jax import lax
from jax.experimental import pallas as pl
from jax.experimental.pallas import tpu as pltpu
from jax.sharding import PartitionSpec as P

HD = 64
SLOT = 1024
MESH = pl.DeviceIdType.MESH


epsilon = 1e-05
rotary_base = 160000.0
masked_score = -1e30


def normalize(values, gain):
    centred = values - jnp.mean(values, axis=-1, keepdims=True)
    factor = lax.rsqrt(jnp.mean(centred * centred, axis=-1, keepdims=True) + epsilon)
    plain = centred * factor
    return (plain, factor, plain * gain)


def normalize_back(change, plain, factor, gain):
    scaled = change * gain
    gain_change = jnp.sum(change * plain, axis=0)
    inner = (
        scaled
        - jnp.mean(scaled, axis=-1, keepdims=True)
        - plain * jnp.mean(scaled * plain, axis=-1, keepdims=True)
    )
    return (factor * inner, gain_change)


def slot_layout(lengths_row, padding_row):
    places = jnp.arange(SLOT, dtype=jnp.int32)
    bounds = jnp.cumsum(lengths_row)
    passed = (places[:, None] >= bounds[None, :]).astype(jnp.int32)
    segment = jnp.sum(passed, axis=1)
    start = jnp.sum(passed * lengths_row[None, :], axis=1)
    position = (places - start).astype(jnp.float32)
    kept = jnp.logical_not(places >= SLOT - padding_row)
    allowed = (segment[:, None] == segment[None, :]) & kept[:, None] & kept[None, :]
    allowed = allowed | (places[:, None] == places[None, :])
    return (position, allowed)


def turning(position):
    halfway = HD // 2
    rates = jnp.exp(jnp.arange(halfway, dtype=jnp.float32) * (-2.0 * math.log(rotary_base) / HD))
    angles = position[:, None] * rates[None, :]
    doubled = jnp.concatenate([angles, angles], axis=1)
    return (jnp.cos(doubled), jnp.sin(doubled))


def rotate(values, cosine, sine):
    halfway = values.shape[-1] // 2
    turned = jnp.concatenate([-values[..., halfway:], values[..., :halfway]], axis=-1)
    return values * cosine[:, None, :] + turned * sine[:, None, :]


def unrotate(change, cosine, sine):
    halfway = change.shape[-1] // 2
    twisted = change * sine[:, None, :]
    turned = jnp.concatenate([twisted[..., halfway:], -twisted[..., :halfway]], axis=-1)
    return change * cosine[:, None, :] + turned


def gelu_slope(inner):
    normal_cdf = 0.5 * (1.0 + lax.erf(inner * (1.0 / math.sqrt(2.0))))
    density = jnp.exp(-0.5 * inner * inner) * (1.0 / math.sqrt(2.0 * math.pi))
    return normal_cdf + inner * density


def slot_scores(packed, lengths_row, padding_row):
    position, allowed = slot_layout(lengths_row, padding_row)
    cosine, sine = turning(position)
    parts = packed.reshape(SLOT, 3, packed.shape[-1] // HD, HD)
    queries = rotate(parts[:, 0].astype(jnp.float32), cosine, sine).astype(jnp.bfloat16)
    keys = rotate(parts[:, 1].astype(jnp.float32), cosine, sine).astype(jnp.bfloat16)
    scores = jnp.einsum("qhd,khd->hqk", queries, keys, preferred_element_type=jnp.float32) * HD ** (
        -0.5
    )
    scores = jnp.where(allowed[None], scores, masked_score)
    return (queries, keys, parts[:, 2], scores, cosine, sine)


def slot_forward(item):
    packed, lengths_row, padding_row = item
    queries, keys, values, scores, cosine, sine = slot_scores(packed, lengths_row, padding_row)
    top = jnp.max(scores, axis=-1, keepdims=True)
    weights = jnp.exp(scores - top)
    total = jnp.sum(weights, axis=-1, keepdims=True)
    probs = (weights / total).astype(jnp.bfloat16)
    mixed = jnp.einsum("hqk,khd->qhd", probs, values, preferred_element_type=jnp.float32)
    return (
        mixed.astype(jnp.bfloat16).reshape(SLOT, packed.shape[-1]),
        (top + jnp.log(total))[..., 0],
    )


def slot_backward(item):
    packed, change_mixed, log_total, lengths_row, padding_row = item
    queries, keys, values, scores, cosine, sine = slot_scores(packed, lengths_row, padding_row)
    share = packed.shape[-1]
    probs = jnp.exp(scores - log_total[..., None])
    change_out = change_mixed.reshape(SLOT, share // HD, HD)
    drift = jnp.einsum("qhd,khd->hqk", change_out, values, preferred_element_type=jnp.float32)
    centre = jnp.sum(probs * drift, axis=-1, keepdims=True)
    score_change = (probs * (drift - centre)).astype(jnp.bfloat16)
    value_change = jnp.einsum(
        "hqk,qhd->khd", probs.astype(jnp.bfloat16), change_out, preferred_element_type=jnp.float32
    )
    query_change = jnp.einsum(
        "hqk,khd->qhd", score_change, keys, preferred_element_type=jnp.float32
    ) * HD ** (-0.5)
    key_change = jnp.einsum(
        "hqk,qhd->khd", score_change, queries, preferred_element_type=jnp.float32
    ) * HD ** (-0.5)
    query_change = unrotate(query_change, cosine, sine)
    key_change = unrotate(key_change, cosine, sine)
    stacked = jnp.stack([query_change, key_change, value_change], axis=1)
    return stacked.astype(jnp.bfloat16).reshape(SLOT, 3, share)


def tiles_of(grad):
    rows, columns = grad.shape
    half = grad.reshape(2, rows // 32, 16, columns // 128, 128)
    return half.transpose(0, 3, 1, 2, 4).reshape(2, -1, 16, 128).astype(jnp.bfloat16)


def grad_of(tiles, rows, columns):
    parts = tiles[: rows * columns // 2048].reshape(columns // 128, rows // 16, 16, 128)
    return parts.transpose(1, 2, 0, 3).reshape(rows, columns).astype(jnp.float32)


class Grid:
    def __init__(self, size):
        self.a = 2 if size < 64 else 4
        self.b = size // (self.a * self.a)
        strides = (1, 32, 4) if size == 128 else (1, self.a, self.a * self.a)
        dp = lax.axis_index("dp")
        core = lax.axis_index("head")
        first = (dp // strides[0]) % self.a
        second = (dp // strides[1]) % self.a
        third = (dp // strides[2]) % self.b
        self.dp, self.core = dp, core
        self.sizes = (self.a, self.a, self.b)
        self.place = (
            first * (1 - core) + second * core,
            second * (1 - core) + first * core,
            third,
        )
        self.stride = (
            strides[0] * (1 - core) + strides[1] * core,
            strides[1] * (1 - core) + strides[0] * core,
            strides[2],
        )

    def peer(self, axis, step):
        index = lax.rem(self.place[axis] + step, self.sizes[axis])
        return index, (self.dp + (index - self.place[axis]) * self.stride[axis], self.core)

    def barrier(self):
        sem = pltpu.get_barrier_semaphore()
        count = 1
        pl.semaphore_signal(sem, inc=1, device_id=(self.dp, 1 - self.core), device_id_type=MESH)
        for axis in range(3):
            for step in range(1, self.sizes[axis]):
                pl.semaphore_signal(sem, inc=1, device_id=self.peer(axis, step)[1], device_id_type=MESH)
                count += 1
        pl.semaphore_wait(sem, count)


def sum_into(out_at, terms, length):
    step = next(n for n in (9, 8, 7, 6, 5, 4, 3, 2, 1) if length % n == 0)

    def body(i, carry):
        at = i * step
        value = terms[0](at, step).astype(jnp.float32)
        for term in terms[1:]:
            value = value + term(at, step).astype(jnp.float32)
        out_at(at, step, value.astype(jnp.bfloat16))
        return carry

    lax.fori_loop(0, length // step, body, 0)


def reader(ref, base=0):
    return lambda at, n: ref[pl.ds(base + at, n)]


def writer(ref, base=0):
    def put(at, n, value):
        ref[pl.ds(base + at, n)] = value

    return put


class Group:
    def __init__(self, grid, tiles, bufs, sends, recvs):
        self.grid, self.tiles = grid, tiles
        self.own, self.got, self.sums, self.whole = bufs
        self.sends, self.recvs = sends, recvs
        self.used = 0
        sizes = grid.sizes
        self.part = (
            tiles // sizes[0],
            tiles // (sizes[0] * sizes[1]),
            tiles // (sizes[0] * sizes[1] * sizes[2]),
        )
        self.flight = []

    def copy(self, source, target, device):
        slot = self.used
        self.used += 1
        copy = pltpu.make_async_remote_copy(
            src_ref=source,
            dst_ref=target,
            send_sem=self.sends.at[slot],
            recv_sem=self.recvs.at[slot],
            device_id=device,
            device_id_type=MESH,
        )
        copy.start()
        self.flight.append(copy)

    def land(self):
        for copy in self.flight:
            copy.wait()
        self.flight = []

    def scatter(self, axis):
        source = self.own if axis == 0 else self.sums[axis - 1]
        part = self.part[axis]
        for step in range(1, self.grid.sizes[axis]):
            index, device = self.grid.peer(axis, step)
            self.copy(
                source.at[pl.ds(index * part, part)], self.got[axis].at[step - 1], device
            )

    def add(self, axis):
        self.land()
        source = self.own if axis == 0 else self.sums[axis - 1]
        part = self.part[axis]
        terms = [reader(source, self.grid.place[axis] * part)]
        for step in range(1, self.grid.sizes[axis]):
            terms.append(reader(self.got[axis].at[step - 1]))
        out = writer(self.sums[axis]) if axis < 2 else writer(self.whole, self.offset(2))
        sum_into(out, terms, part)

    def offset(self, axis):
        return sum(self.grid.place[k] * self.part[k] for k in range(axis + 1))

    def gather(self, axis):
        block = self.whole.at[pl.ds(self.offset(axis), self.part[axis])]
        for step in range(1, self.grid.sizes[axis]):
            self.copy(block, block, self.grid.peer(axis, step)[1])

    def stages(self):
        def first():
            self.scatter(0)

        def turn(axis):
            def run():
                self.add(axis)
                if axis < 2:
                    self.scatter(axis + 1)
                else:
                    self.gather(2)

            return run

        def spread(axis):
            def run():
                self.land()
                self.gather(axis)

            return run

        return [first, turn(0), turn(1), turn(2), spread(1), spread(0), self.land]


def group_scratch(tiles, size):
    a = 2 if size < 64 else 4
    b = size // (a * a)
    shape = lambda *s: pltpu.VMEM(s + (16, 128), jnp.bfloat16)
    copies = 2 * (2 * (a - 1) + (b - 1))
    return [
        shape(a - 1, tiles // a),
        shape(a - 1, tiles // (a * a)),
        shape(b - 1, tiles // size),
        shape(tiles // a),
        shape(tiles // (a * a)),
        pltpu.SemaphoreType.DMA((copies,)),
        pltpu.SemaphoreType.DMA((copies,)),
    ]


def reduce_kernel(size, counts, *refs):
    total = len(counts)
    ins, refs = refs[:total], refs[total:]
    vec_in, refs = refs[0], refs[1:]
    outs, refs = refs[:total], refs[total:]
    vec_out, refs = refs[0], refs[1:]
    grid = Grid(size)
    pair_send, pair_recv, vec_send, vec_recv, vec_got, refs = refs[0], refs[1], refs[2], refs[3], refs[4], refs[5:]
    owns, refs = refs[:total], refs[total:]
    theirs, refs = refs[:total], refs[total:]
    grid.barrier()
    pair = (grid.dp, 1 - grid.core)
    copies = []
    for k in range(total):
        copy = pltpu.make_async_remote_copy(
            src_ref=ins[k].at[1 - grid.core],
            dst_ref=theirs[k],
            send_sem=pair_send.at[k],
            recv_sem=pair_recv.at[k],
            device_id=pair,
            device_id_type=MESH,
        )
        copy.start()
        copies.append(copy)
    plans = []
    for k in range(total):
        own = refs[7 * k : 7 * k + 7]
        group = Group(
            grid, counts[k], (owns[k], own[0:3], own[3:5], outs[k]), own[5], own[6]
        )

        def join(k=k, group=group):
            copies[k].wait()
            sum_into(
                writer(owns[k]),
                [reader(ins[k].at[grid.core]), reader(theirs[k])],
                counts[k],
            )

        plans.append([join] + group.stages())
    depth = len(plans[0])
    for moment in range(depth + total - 1):
        for k in range(total - 1, -1, -1):
            if 0 <= moment - k < depth:
                plans[k][moment - k]()
    vec_out[...] = vec_in[...]
    slot = 0
    legs = [[pair]] + [
        [grid.peer(axis, step)[1] for step in range(1, grid.sizes[axis])] for axis in range(3)
    ]
    for leg in legs:
        flight = []
        vec_got[slot, :, :] = vec_out[...]
        for j, device in enumerate(leg):
            copy = pltpu.make_async_remote_copy(
                src_ref=vec_got.at[slot],
                dst_ref=vec_got.at[slot + 1 + j],
                send_sem=vec_send.at[slot + j],
                recv_sem=vec_recv.at[slot + j],
                device_id=device,
                device_id_type=MESH,
            )
            copy.start()
            flight.append(copy)
        for copy in flight:
            copy.wait()
        value = vec_got[slot]
        for j in range(len(leg)):
            value = value + vec_got[slot + 1 + j]
        vec_out[...] = value
        slot += len(leg) + 1


def reduce_gradients(mixer_grad, joined_grad, merge_grad, feeder_grad, expand_grad, shrink_grad):
    size = lax.axis_size("dp")
    core = lax.axis_index("head")

    def padded(tiles):
        extra = -tiles.shape[1] % size
        return jnp.pad(tiles, ((0, 0), (0, extra), (0, 0), (0, 0)))

    ins = [padded(tiles_of(shrink_grad))]
    for j in range(3):
        ins.append(padded(tiles_of(expand_grad[:, 768 * j : 768 * j + 768])))
    ins.append(padded(tiles_of(merge_grad)))
    for j in range(3):
        ins.append(padded(tiles_of(joined_grad[:, 768 * j : 768 * j + 768])))
    counts = [i.shape[1] for i in ins]
    vec = jnp.concatenate([mixer_grad.reshape(6, 128), feeder_grad.reshape(6, 128), jnp.zeros((4, 128))])
    vmem = pl.BlockSpec(memory_space=pltpu.VMEM)
    tile = lambda n: (n, 16, 128)
    total = len(ins)
    a = 2 if size < 64 else 4
    b = size // (a * a)
    slots = 1 + 2 * (a - 1) + (b - 1) + 4
    scratch = [
        pltpu.SemaphoreType.DMA((total,)),
        pltpu.SemaphoreType.DMA((total,)),
        pltpu.SemaphoreType.DMA((slots,)),
        pltpu.SemaphoreType.DMA((slots,)),
        pltpu.VMEM((slots, 16, 128), jnp.float32),
    ]
    scratch += [pltpu.VMEM(tile(n), jnp.bfloat16) for n in counts]
    scratch += [pltpu.VMEM(tile(n), jnp.bfloat16) for n in counts]
    for n in counts:
        scratch += group_scratch(n, size)
    outs = pl.pallas_call(
        functools.partial(reduce_kernel, size, counts),
        out_shape=[jax.ShapeDtypeStruct(tile(n), jnp.bfloat16) for n in counts]
        + [jax.ShapeDtypeStruct((16, 128), jnp.float32)],
        in_specs=[vmem] * (total + 1),
        out_specs=[vmem] * (total + 1),
        scratch_shapes=scratch,
        compiler_params=pltpu.CompilerParams(
            collective_id=0, has_side_effects=True, vmem_limit_bytes=62 << 20
        ),
    )(*ins, vec)
    vec_sum = outs[-1]
    mixer = lax.dynamic_slice(vec_sum[:6].reshape(768), (core * 384,), (384,))
    feeder = lax.dynamic_slice(vec_sum[6:12].reshape(768), (core * 384,), (384,))
    expand = jnp.concatenate([grad_of(outs[j], 384, 768) for j in (1, 2, 3)], axis=1)
    joined = jnp.concatenate([grad_of(outs[j], 384, 768) for j in (5, 6, 7)], axis=1)
    return (
        mixer,
        joined,
        grad_of(outs[4], 384, 768),
        feeder,
        expand,
        grad_of(outs[0], 576, 768),
    )


def shards(
    tokens,
    mixer_gain,
    joined_weight,
    merge_weight,
    feeder_gain,
    expand_weight,
    shrink_weight,
    doc_lengths,
    padding,
    cotangent,
):
    group = lax.axis_size("head")
    rows = tokens.shape[0]
    width = tokens.shape[1]
    share = width // group
    slots = rows * group // SLOT
    hidden_width = shrink_weight.shape[0]
    inputs = tokens.astype(jnp.float32)
    plain_one, factor_one, normed_one = normalize(inputs, mixer_gain)
    first_in = normed_one.astype(jnp.bfloat16)
    joined = jnp.dot(first_in, joined_weight, preferred_element_type=jnp.float32).astype(
        jnp.bfloat16
    )
    spread = lax.all_to_all(
        joined.reshape(rows, 3, group, share), "head", split_axis=2, concat_axis=0, tiled=True
    )
    packed = spread.reshape(slots, SLOT, 3, share)
    mixed_heads, log_totals = lax.map(slot_forward, (packed, doc_lengths, padding))
    mixed_back = lax.all_to_all(
        mixed_heads.reshape(rows * group, 1, share), "head", split_axis=0, concat_axis=1, tiled=True
    )
    mixed = mixed_back.reshape(rows, width)
    residual = inputs + jnp.dot(mixed, merge_weight, preferred_element_type=jnp.float32)
    plain_two, factor_two, normed_two = normalize(residual, feeder_gain)
    second_in = normed_two.astype(jnp.bfloat16)
    expanded = jnp.dot(second_in, expand_weight, preferred_element_type=jnp.float32)
    inner = expanded[:, :hidden_width]
    gate = expanded[:, hidden_width:]
    activated = jax.nn.gelu(inner, approximate=False)
    hidden = (activated * gate).astype(jnp.bfloat16)
    block_output = (
        residual + jnp.dot(hidden, shrink_weight, preferred_element_type=jnp.float32)
    ).astype(jnp.bfloat16)
    shrink_grad = jnp.dot(hidden.T, cotangent, preferred_element_type=jnp.float32)
    hidden_change = jnp.dot(cotangent, shrink_weight.T, preferred_element_type=jnp.float32)
    expand_change = jnp.concatenate(
        [hidden_change * gate * gelu_slope(inner), hidden_change * activated], axis=1
    ).astype(jnp.bfloat16)
    expand_grad = jnp.dot(second_in.T, expand_change, preferred_element_type=jnp.float32)
    second_change = jnp.dot(expand_change, expand_weight.T, preferred_element_type=jnp.float32)
    residual_part, feeder_grad = normalize_back(second_change, plain_two, factor_two, feeder_gain)
    residual_change = cotangent.astype(jnp.float32) + residual_part
    residual_low = residual_change.astype(jnp.bfloat16)
    merge_grad = jnp.dot(mixed.T, residual_low, preferred_element_type=jnp.float32)
    mixed_change = jnp.dot(residual_low, merge_weight.T, preferred_element_type=jnp.float32).astype(
        jnp.bfloat16
    )
    change_heads = lax.all_to_all(
        mixed_change.reshape(rows, group, share), "head", split_axis=1, concat_axis=0, tiled=True
    )
    head_changes = lax.map(
        slot_backward,
        (packed, change_heads.reshape(slots, SLOT, share), log_totals, doc_lengths, padding),
    )
    returned = lax.all_to_all(
        head_changes.reshape(rows * group, 3, 1, share),
        "head",
        split_axis=0,
        concat_axis=2,
        tiled=True,
    )
    joined_change = returned.reshape(rows, 3 * width)
    joined_grad = jnp.dot(first_in.T, joined_change, preferred_element_type=jnp.float32)
    first_change = jnp.dot(joined_change, joined_weight.T, preferred_element_type=jnp.float32)
    input_part, mixer_grad = normalize_back(first_change, plain_one, factor_one, mixer_gain)
    tokens_gradient = (residual_change + input_part).astype(jnp.bfloat16)
    total = reduce_gradients(
        mixer_grad, joined_grad, merge_grad, feeder_grad, expand_grad, shrink_grad
    )
    return (block_output, tokens_gradient) + total


def solution(mesh):
    in_specs = (
        P(("dp", "head"), None),
        P(),
        P(),
        P(),
        P(),
        P(),
        P(),
        P("dp", None),
        P("dp"),
        P(("dp", "head"), None),
    )
    out_specs = (
        P(("dp", "head"), None),
        P(("dp", "head"), None),
        P("head"),
        P("head", None),
        P("head", None),
        P("head"),
        P("head", None),
        P("head", None),
    )
    return jax.shard_map(shards, mesh=mesh, in_specs=in_specs, out_specs=out_specs, check_vma=False)
```

```python
import functools
import math

import jax
import jax.numpy as jnp
from jax import lax
from jax.experimental import pallas as pl
from jax.experimental.pallas import tpu as pltpu
from jax.sharding import PartitionSpec as P

HD = 64
SLOT = 1024
MESH = pl.DeviceIdType.MESH


epsilon = 1e-05
rotary_base = 160000.0
masked_score = -1e30


def normalize(values, gain):
    centred = values - jnp.mean(values, axis=-1, keepdims=True)
    factor = lax.rsqrt(jnp.mean(centred * centred, axis=-1, keepdims=True) + epsilon)
    plain = centred * factor
    return (plain, factor, plain * gain)


def normalize_back(change, plain, factor, gain):
    scaled = change * gain
    gain_change = jnp.sum(change * plain, axis=0)
    inner = (
        scaled
        - jnp.mean(scaled, axis=-1, keepdims=True)
        - plain * jnp.mean(scaled * plain, axis=-1, keepdims=True)
    )
    return (factor * inner, gain_change)


def slot_layout(lengths_row, padding_row):
    places = jnp.arange(SLOT, dtype=jnp.int32)
    bounds = jnp.cumsum(lengths_row)
    passed = (places[:, None] >= bounds[None, :]).astype(jnp.int32)
    segment = jnp.sum(passed, axis=1)
    start = jnp.sum(passed * lengths_row[None, :], axis=1)
    position = (places - start).astype(jnp.float32)
    kept = jnp.logical_not(places >= SLOT - padding_row)
    allowed = (segment[:, None] == segment[None, :]) & kept[:, None] & kept[None, :]
    allowed = allowed | (places[:, None] == places[None, :])
    return (position, allowed)


def turning(position):
    halfway = HD // 2
    rates = jnp.exp(jnp.arange(halfway, dtype=jnp.float32) * (-2.0 * math.log(rotary_base) / HD))
    angles = position[:, None] * rates[None, :]
    doubled = jnp.concatenate([angles, angles], axis=1)
    return (jnp.cos(doubled), jnp.sin(doubled))


def rotate(values, cosine, sine):
    halfway = values.shape[-1] // 2
    turned = jnp.concatenate([-values[..., halfway:], values[..., :halfway]], axis=-1)
    return values * cosine[:, None, :] + turned * sine[:, None, :]


def unrotate(change, cosine, sine):
    halfway = change.shape[-1] // 2
    twisted = change * sine[:, None, :]
    turned = jnp.concatenate([twisted[..., halfway:], -twisted[..., :halfway]], axis=-1)
    return change * cosine[:, None, :] + turned


def gelu_slope(inner):
    normal_cdf = 0.5 * (1.0 + lax.erf(inner * (1.0 / math.sqrt(2.0))))
    density = jnp.exp(-0.5 * inner * inner) * (1.0 / math.sqrt(2.0 * math.pi))
    return normal_cdf + inner * density


def slot_scores(packed, lengths_row, padding_row):
    position, allowed = slot_layout(lengths_row, padding_row)
    cosine, sine = turning(position)
    parts = packed.reshape(SLOT, 3, packed.shape[-1] // HD, HD)
    queries = rotate(parts[:, 0].astype(jnp.float32), cosine, sine).astype(jnp.bfloat16)
    keys = rotate(parts[:, 1].astype(jnp.float32), cosine, sine).astype(jnp.bfloat16)
    scores = jnp.einsum("qhd,khd->hqk", queries, keys, preferred_element_type=jnp.float32) * HD ** (
        -0.5
    )
    scores = jnp.where(allowed[None], scores, masked_score)
    return (queries, keys, parts[:, 2], scores, cosine, sine)


def slot_forward(item):
    packed, lengths_row, padding_row = item
    queries, keys, values, scores, cosine, sine = slot_scores(packed, lengths_row, padding_row)
    top = jnp.max(scores, axis=-1, keepdims=True)
    weights = jnp.exp(scores - top)
    total = jnp.sum(weights, axis=-1, keepdims=True)
    probs = (weights / total).astype(jnp.bfloat16)
    mixed = jnp.einsum("hqk,khd->qhd", probs, values, preferred_element_type=jnp.float32)
    return (
        mixed.astype(jnp.bfloat16).reshape(SLOT, packed.shape[-1]),
        (top + jnp.log(total))[..., 0],
    )


def slot_backward(item):
    packed, change_mixed, log_total, lengths_row, padding_row = item
    queries, keys, values, scores, cosine, sine = slot_scores(packed, lengths_row, padding_row)
    share = packed.shape[-1]
    probs = jnp.exp(scores - log_total[..., None])
    change_out = change_mixed.reshape(SLOT, share // HD, HD)
    drift = jnp.einsum("qhd,khd->hqk", change_out, values, preferred_element_type=jnp.float32)
    centre = jnp.sum(probs * drift, axis=-1, keepdims=True)
    score_change = (probs * (drift - centre)).astype(jnp.bfloat16)
    value_change = jnp.einsum(
        "hqk,qhd->khd", probs.astype(jnp.bfloat16), change_out, preferred_element_type=jnp.float32
    )
    query_change = jnp.einsum(
        "hqk,khd->qhd", score_change, keys, preferred_element_type=jnp.float32
    ) * HD ** (-0.5)
    key_change = jnp.einsum(
        "hqk,qhd->khd", score_change, queries, preferred_element_type=jnp.float32
    ) * HD ** (-0.5)
    query_change = unrotate(query_change, cosine, sine)
    key_change = unrotate(key_change, cosine, sine)
    stacked = jnp.stack([query_change, key_change, value_change], axis=1)
    return stacked.astype(jnp.bfloat16).reshape(SLOT, 3, share)


class Grid:
    def __init__(self, size):
        self.a = 2 if size < 64 else 4
        self.b = size // (self.a * self.a)
        strides = (1, 32, 4) if size == 128 else (1, self.a, self.a * self.a)
        dp = lax.axis_index("dp")
        core = lax.axis_index("head")
        first = (dp // strides[0]) % self.a
        second = (dp // strides[1]) % self.a
        third = (dp // strides[2]) % self.b
        self.dp, self.core = dp, core
        self.sizes = (self.a, self.a, self.b)
        self.place = (
            first * (1 - core) + second * core,
            second * (1 - core) + first * core,
            third,
        )
        self.stride = (
            strides[0] * (1 - core) + strides[1] * core,
            strides[1] * (1 - core) + strides[0] * core,
            strides[2],
        )

    def peer(self, axis, step):
        index = lax.rem(self.place[axis] + step, self.sizes[axis])
        return index, (self.dp + (index - self.place[axis]) * self.stride[axis], self.core)

    def barrier(self):
        sem = pltpu.get_barrier_semaphore()
        count = 1
        pl.semaphore_signal(sem, inc=1, device_id=(self.dp, 1 - self.core), device_id_type=MESH)
        for axis in range(3):
            for step in range(1, self.sizes[axis]):
                pl.semaphore_signal(sem, inc=1, device_id=self.peer(axis, step)[1], device_id_type=MESH)
                count += 1
        pl.semaphore_wait(sem, count)


def sum_into(out_at, terms, length):
    step = next(n for n in (9, 8, 7, 6, 5, 4, 3, 2, 1) if length % n == 0)

    def body(i, carry):
        at = i * step
        value = terms[0](at, step).astype(jnp.float32)
        for term in terms[1:]:
            value = value + term(at, step).astype(jnp.float32)
        out_at(at, step, value.astype(jnp.bfloat16))
        return carry

    lax.fori_loop(0, length // step, body, 0)


def reader(ref, base=0):
    return lambda at, n: ref[pl.ds(base + at, n)]


def writer(ref, base=0):
    def put(at, n, value):
        ref[pl.ds(base + at, n)] = value

    return put


class Group:
    def __init__(self, grid, tiles, bufs, sends, recvs):
        self.grid, self.tiles = grid, tiles
        self.own, self.got, self.sums, self.whole = bufs
        self.sends, self.recvs = sends, recvs
        self.used = 0
        sizes = grid.sizes
        self.part = (
            tiles // sizes[0],
            tiles // (sizes[0] * sizes[1]),
            tiles // (sizes[0] * sizes[1] * sizes[2]),
        )
        self.flight = []

    def copy(self, source, target, device):
        slot = self.used
        self.used += 1
        copy = pltpu.make_async_remote_copy(
            src_ref=source,
            dst_ref=target,
            send_sem=self.sends.at[slot],
            recv_sem=self.recvs.at[slot],
            device_id=device,
            device_id_type=MESH,
        )
        copy.start()
        self.flight.append(copy)

    def land(self):
        for copy in self.flight:
            copy.wait()
        self.flight = []

    def scatter(self, axis):
        source = self.own if axis == 0 else self.sums[axis - 1]
        part = self.part[axis]
        for step in range(1, self.grid.sizes[axis]):
            index, device = self.grid.peer(axis, step)
            self.copy(
                source.at[pl.ds(index * part, part)], self.got[axis].at[step - 1], device
            )

    def add(self, axis):
        self.land()
        source = self.own if axis == 0 else self.sums[axis - 1]
        part = self.part[axis]
        terms = [reader(source, self.grid.place[axis] * part)]
        for step in range(1, self.grid.sizes[axis]):
            terms.append(reader(self.got[axis].at[step - 1]))
        out = writer(self.sums[axis]) if axis < 2 else writer(self.whole, self.offset(2))
        sum_into(out, terms, part)

    def offset(self, axis):
        return sum(self.grid.place[k] * self.part[k] for k in range(axis + 1))

    def gather(self, axis):
        block = self.whole.at[pl.ds(self.offset(axis), self.part[axis])]
        for step in range(1, self.grid.sizes[axis]):
            self.copy(block, block, self.grid.peer(axis, step)[1])

    def stages(self):
        def first():
            self.scatter(0)

        def turn(axis):
            def run():
                self.add(axis)
                if axis < 2:
                    self.scatter(axis + 1)
                else:
                    self.gather(2)

            return run

        def spread(axis):
            def run():
                self.land()
                self.gather(axis)

            return run

        return [first, turn(0), turn(1), turn(2), spread(1), spread(0), self.land]


def group_scratch(tiles, size):
    a = 2 if size < 64 else 4
    b = size // (a * a)
    shape = lambda *s: pltpu.VMEM(s + (16, 128), jnp.bfloat16)
    copies = 2 * (2 * (a - 1) + (b - 1))
    return [
        shape(a - 1, tiles // a),
        shape(a - 1, tiles // (a * a)),
        shape(b - 1, tiles // size),
        shape(tiles // a),
        shape(tiles // (a * a)),
        pltpu.SemaphoreType.DMA((copies,)),
        pltpu.SemaphoreType.DMA((copies,)),
    ]


def reduce_kernel(size, plan, counts, *refs):
    total = len(plan)
    ins, refs = refs[:8], refs[8:]
    vec_in, refs = refs[0], refs[1:]
    outs, refs = refs[:4], refs[4:]
    vec_out, refs = refs[0], refs[1:]
    grid = Grid(size)
    pair_send, pair_recv, vec_send, vec_recv, vec_got, flipped = refs[:6]
    refs = refs[6:]
    owns, refs = refs[:total], refs[total:]
    gives, refs = refs[:total], refs[total:]
    theirs, refs = refs[:total], refs[total:]
    wholes, refs = refs[:total], refs[total:]
    grid.barrier()
    pair = (grid.dp, 1 - grid.core)
    plans = []
    held = [None]
    for k in range(total):
        left, right, column, target = plan[k]
        rows = ins[left].shape[1] // 2
        own = refs[7 * k : 7 * k + 7]
        group = Group(
            grid, counts[k], (owns[k], own[0:3], own[3:5], wholes[k]), own[5], own[6]
        )

        def product(half, into, left=left, right=right, column=column, rows=rows):
            def body(i, carry):
                at = pl.multiple_of(column + i * 256, 256)
                block = jnp.dot(
                    flipped[pl.ds(pl.multiple_of(half * rows, 16), rows), :],
                    ins[right][:, pl.ds(at, 256)],
                    preferred_element_type=jnp.float32,
                ).astype(jnp.bfloat16)
                for part in range(2):
                    into[pl.ds((2 * i + part) * (rows // 16), rows // 16)] = block[
                        :, part * 128 : part * 128 + 128
                    ].reshape(rows // 16, 16, 128)
                return carry

            lax.fori_loop(0, 3, body, 0)

        pending = []

        def make(k=k, left=left, product=product, pending=pending, rows=rows):
            if held[0] != left:
                flipped[: 2 * rows, :] = ins[left][...].T
                held[0] = left
            product(1 - grid.core, gives[k])
            copy = pltpu.make_async_remote_copy(
                src_ref=gives[k],
                dst_ref=theirs[k],
                send_sem=pair_send.at[k],
                recv_sem=pair_recv.at[k],
                device_id=pair,
                device_id_type=MESH,
            )
            copy.start()
            pending.append(copy)
            product(grid.core, owns[k])

        def join(k=k, group=group, pending=pending):
            pending[0].wait()
            used = theirs[k].shape[0]
            sum_into(writer(owns[k]), [reader(owns[k]), reader(theirs[k])], used)
            if used < counts[k]:
                owns[k][used:] = jnp.zeros((counts[k] - used, 16, 128), jnp.bfloat16)

        def finish(k=k, column=column, target=target, rows=rows, group=group):
            group.land()

            def body(i, carry):
                block = wholes[k][pl.ds(i * (rows // 16), rows // 16)]
                outs[target][:, pl.ds(pl.multiple_of(column + i * 128, 128), 128)] = (
                    block.reshape(rows, 128).astype(jnp.float32)
                )
                return carry

            lax.fori_loop(0, 6, body, 0)

        plans.append([make, join] + group.stages()[:-1] + [finish])
    depth = len(plans[0])
    for moment in range(depth + total - 1):
        for k in range(total):
            if 0 <= moment - k < depth:
                plans[k][moment - k]()
    vec_out[...] = vec_in[...]
    slot = 0
    legs = [[pair]] + [
        [grid.peer(axis, step)[1] for step in range(1, grid.sizes[axis])] for axis in range(3)
    ]
    for leg in legs:
        flight = []
        vec_got[slot, :, :] = vec_out[...]
        for j, device in enumerate(leg):
            copy = pltpu.make_async_remote_copy(
                src_ref=vec_got.at[slot],
                dst_ref=vec_got.at[slot + 1 + j],
                send_sem=vec_send.at[slot + j],
                recv_sem=vec_recv.at[slot + j],
                device_id=device,
                device_id_type=MESH,
            )
            copy.start()
            flight.append(copy)
        for copy in flight:
            copy.wait()
        value = vec_got[slot]
        for j in range(len(leg)):
            value = value + vec_got[slot + 1 + j]
        vec_out[...] = value
        slot += len(leg) + 1


def reduce_gradients(pairs, mixer_grad, feeder_grad):
    size = lax.axis_size("dp")
    core = lax.axis_index("head")
    ins = [array for pair in pairs for array in pair]
    plan = [(2, 3, 0, 1), (2, 3, 768, 1), (2, 3, 1536, 1), (0, 1, 0, 0), (4, 5, 0, 2)]
    plan += [(6, 7, 0, 3), (6, 7, 768, 3), (6, 7, 1536, 3)]
    real = [ins[left].shape[1] // 2 * 768 // 2048 for left, _, _, _ in plan]
    counts = [n + -n % size for n in real]
    vec = jnp.concatenate([mixer_grad.reshape(6, 128), feeder_grad.reshape(6, 128), jnp.zeros((4, 128))])
    vmem = pl.BlockSpec(memory_space=pltpu.VMEM)
    tile = lambda n: pltpu.VMEM((n, 16, 128), jnp.bfloat16)
    total = len(plan)
    a = 2 if size < 64 else 4
    b = size // (a * a)
    slots = 1 + 2 * (a - 1) + (b - 1) + 4
    scratch = [
        pltpu.SemaphoreType.DMA((total,)),
        pltpu.SemaphoreType.DMA((total,)),
        pltpu.SemaphoreType.DMA((slots,)),
        pltpu.SemaphoreType.DMA((slots,)),
        pltpu.VMEM((slots, 16, 128), jnp.float32),
        pltpu.VMEM((max(i.shape[1] for i in ins[::2]), ins[0].shape[0]), jnp.bfloat16),
    ]
    scratch += [tile(n) for n in counts] + [tile(n) for n in real]
    scratch += [tile(n) for n in real] + [tile(n) for n in counts]
    for n in counts:
        scratch += group_scratch(n, size)
    outs = pl.pallas_call(
        functools.partial(reduce_kernel, size, plan, counts),
        out_shape=[
            jax.ShapeDtypeStruct((left.shape[1] // 2, right.shape[1]), jnp.float32)
            for left, right in pairs
        ]
        + [jax.ShapeDtypeStruct((16, 128), jnp.float32)],
        in_specs=[vmem] * (len(ins) + 1),
        out_specs=[vmem] * 5,
        scratch_shapes=scratch,
        compiler_params=pltpu.CompilerParams(
            collective_id=0, has_side_effects=True, vmem_limit_bytes=63 << 20
        ),
    )(*ins, vec)
    vec_sum = outs[-1]
    mixer = lax.dynamic_slice(vec_sum[:6].reshape(768), (core * 384,), (384,))
    feeder = lax.dynamic_slice(vec_sum[6:12].reshape(768), (core * 384,), (384,))
    return (mixer, outs[3], outs[2], feeder, outs[1], outs[0])


def shards(
    tokens,
    mixer_gain,
    joined_weight,
    merge_weight,
    feeder_gain,
    expand_weight,
    shrink_weight,
    doc_lengths,
    padding,
    cotangent,
):
    group = lax.axis_size("head")
    rows = tokens.shape[0]
    width = tokens.shape[1]
    share = width // group
    slots = rows * group // SLOT
    hidden_width = shrink_weight.shape[0]
    inputs = tokens.astype(jnp.float32)
    plain_one, factor_one, normed_one = normalize(inputs, mixer_gain)
    first_in = normed_one.astype(jnp.bfloat16)
    joined = jnp.dot(first_in, joined_weight, preferred_element_type=jnp.float32).astype(
        jnp.bfloat16
    )
    spread = lax.all_to_all(
        joined.reshape(rows, 3, group, share), "head", split_axis=2, concat_axis=0, tiled=True
    )
    packed = spread.reshape(slots, SLOT, 3, share)
    mixed_heads, log_totals = lax.map(slot_forward, (packed, doc_lengths, padding))
    mixed_back = lax.all_to_all(
        mixed_heads.reshape(rows * group, 1, share), "head", split_axis=0, concat_axis=1, tiled=True
    )
    mixed = mixed_back.reshape(rows, width)
    residual = inputs + jnp.dot(mixed, merge_weight, preferred_element_type=jnp.float32)
    plain_two, factor_two, normed_two = normalize(residual, feeder_gain)
    second_in = normed_two.astype(jnp.bfloat16)
    expanded = jnp.dot(second_in, expand_weight, preferred_element_type=jnp.float32)
    inner = expanded[:, :hidden_width]
    gate = expanded[:, hidden_width:]
    activated = jax.nn.gelu(inner, approximate=False)
    hidden = (activated * gate).astype(jnp.bfloat16)
    block_output = (
        residual + jnp.dot(hidden, shrink_weight, preferred_element_type=jnp.float32)
    ).astype(jnp.bfloat16)
    hidden_change = jnp.dot(cotangent, shrink_weight.T, preferred_element_type=jnp.float32)
    expand_change = jnp.concatenate(
        [hidden_change * gate * gelu_slope(inner), hidden_change * activated], axis=1
    ).astype(jnp.bfloat16)
    second_change = jnp.dot(expand_change, expand_weight.T, preferred_element_type=jnp.float32)
    residual_part, feeder_grad = normalize_back(second_change, plain_two, factor_two, feeder_gain)
    residual_change = cotangent.astype(jnp.float32) + residual_part
    residual_low = residual_change.astype(jnp.bfloat16)
    mixed_change = jnp.dot(residual_low, merge_weight.T, preferred_element_type=jnp.float32).astype(
        jnp.bfloat16
    )
    change_heads = lax.all_to_all(
        mixed_change.reshape(rows, group, share), "head", split_axis=1, concat_axis=0, tiled=True
    )
    head_changes = lax.map(
        slot_backward,
        (packed, change_heads.reshape(slots, SLOT, share), log_totals, doc_lengths, padding),
    )
    returned = lax.all_to_all(
        head_changes.reshape(rows * group, 3, 1, share),
        "head",
        split_axis=0,
        concat_axis=2,
        tiled=True,
    )
    joined_change = returned.reshape(rows, 3 * width)
    first_change = jnp.dot(joined_change, joined_weight.T, preferred_element_type=jnp.float32)
    input_part, mixer_grad = normalize_back(first_change, plain_one, factor_one, mixer_gain)
    tokens_gradient = (residual_change + input_part).astype(jnp.bfloat16)
    pairs = (
        (hidden, cotangent),
        (second_in, expand_change),
        (mixed, residual_low),
        (first_in, joined_change),
    )
    total = reduce_gradients(pairs, mixer_grad, feeder_grad)
    return (block_output, tokens_gradient) + total


def solution(mesh):
    in_specs = (
        P(("dp", "head"), None),
        P(),
        P(),
        P(),
        P(),
        P(),
        P(),
        P("dp", None),
        P("dp"),
        P(("dp", "head"), None),
    )
    out_specs = (
        P(("dp", "head"), None),
        P(("dp", "head"), None),
        P("head"),
        P("head", None),
        P("head", None),
        P("head"),
        P("head", None),
        P("head", None),
    )
    return jax.shard_map(shards, mesh=mesh, in_specs=in_specs, out_specs=out_specs, check_vma=False)
```
